16 devices in a mesh: rep: 4 (over y, z, core), dp: 4 (over x).
Axes of the slice: x: 4, y: 2, z: 1, core: 2. Of those that a mesh axis runs over, the one named last changes fastest.
The devices are a block of a 4x4x8 slice.
Arguments:
- x: bfloat16 [16, 4096, 512], P(('rep', 'dp')), parts along dimension 0
- dy: bfloat16 [16, 4096, 512], P(('rep', 'dp')), parts along dimension 0
- w_gate: bfloat16 [2, 512, 4096], replicated
- w_up: bfloat16 [2, 512, 4096], replicated
- w_down: bfloat16 [2, 4096, 512], replicated
- m_w_gate: float32 [2, 512, 4096], P(None, 'dp')
- m_w_up: float32 [2, 512, 4096], P(None, 'dp')
- m_w_down: float32 [2, 4096, 512], P(None, 'dp')
- v_w_gate: float32 [2, 512, 4096], P(None, 'dp')
- v_w_up: float32 [2, 512, 4096], P(None, 'dp')
- v_w_down: float32 [2, 4096, 512], P(None, 'dp')
Outputs:
- output 1: bfloat16 [8, 512, 4096], P('rep'), parts along dimension 0
- output 2: bfloat16 [8, 512, 4096], P('rep'), parts along dimension 0
- output 3: bfloat16 [8, 4096, 512], P('rep'), parts along dimension 0
- output 4: float32 [8, 512, 4096], P('rep', 'dp'), parts along dimension 0
- output 5: float32 [8, 512, 4096], P('rep', 'dp'), parts along dimension 0
- output 6: float32 [8, 4096, 512], P('rep', 'dp'), parts along dimension 0
- output 7: float32 [8, 512, 4096], P('rep', 'dp'), parts along dimension 0
- output 8: float32 [8, 512, 4096], P('rep', 'dp'), parts along dimension 0
- output 9: float32 [8, 4096, 512], P('rep', 'dp'), parts along dimension 0
There are 4 independent parts. The reference program is written for one: setup_inputs(seed, part) draws one part's arguments, and reference() takes and returns one part's arrays. A program takes and returns all parts, laid end to end along the dimension named above; an argument that names none is the same for every part.
All inputs are finite; a program needn't handle non-finite values.
Results may differ from the reference program's by a relative error of at most 0.022.
Values are sent between devices in bfloat16 or wider.
A program may use at most 768 MiB of HBM per device.

```python
import jax
import jax.numpy as jnp
from jax import lax

SEQUENCES = 4
TOKENS = 4096
D = 512
FF = 4096
LAYERS = 2
NAMES = ("w_gate", "w_up", "w_down")
SHAPES = {"w_gate": (LAYERS, D, FF), "w_up": (LAYERS, D, FF), "w_down": (LAYERS, FF, D)}


def bump(key, n, height):
    away = (jnp.arange(n, dtype=jnp.int32) - jax.random.randint(key, (), 0, n, jnp.int32)) % n
    return jnp.where(away < n // 8, height, 1.0)


def together(key, own, strength):
    shared = jax.random.normal(key, own.shape[1:], jnp.float32)
    return (own + strength * shared) * lax.rsqrt(1 + strength * strength)


def setup_inputs(seed: int = 0, part: int = 0) -> dict:
    kx, kdy, ka, kb, kz, kf, kh, kl, *keys = jax.random.split(jax.random.key(seed), 8 + 3 * len(NAMES))
    kx, kdy, ka, kb = (jax.random.fold_in(k, part) for k in (kx, kdy, ka, kb))
    kw, km, kv = (keys[i::3] for i in range(3))
    shape = (SEQUENCES, TOKENS, D)
    much_x, much_dy = jax.random.uniform(kz, (2,), jnp.float32, 0.0, 1.0)
    loud = 2.0 ** jax.random.uniform(jax.random.fold_in(kz, 1), (), jnp.float32, -1.0, 2.0)
    layers = 2.0 ** jax.random.uniform(kl, (LAYERS, 1, 1), jnp.float32, -1.0, 1.0)
    x = together(ka, jax.random.normal(kx, shape, jnp.float32), much_x) * bump(kf, D, 4.0)
    dy = together(kb, jax.random.normal(kdy, shape, jnp.float32), much_dy)
    drawn = {"x": x.astype(jnp.bfloat16), "dy": (loud * dy * (SEQUENCES * TOKENS) ** -0.5).astype(jnp.bfloat16)}
    for key, name in zip(kw, NAMES, strict=True):
        w = jax.random.normal(key, SHAPES[name], jnp.float32) * SHAPES[name][1] ** -0.5
        drawn[name] = (w * {"w_gate": 1.0, "w_up": bump(kh, FF, 4.0), "w_down": layers}[name]).astype(jnp.bfloat16)
    for key, name in zip(km, NAMES, strict=True):
        drawn[f"m_{name}"] = 0.1 * jax.random.normal(key, SHAPES[name], jnp.float32)
    for key, name in zip(kv, NAMES, strict=True):
        drawn[f"v_{name}"] = jax.random.uniform(key, SHAPES[name], jnp.float32, 0.005, 0.015)
    return drawn


def matmul(a, w):
    return jnp.dot(a, w, preferred_element_type=jnp.float32).astype(jnp.bfloat16)


def normed(h):
    wide = h.astype(jnp.float32)
    scale = lax.rsqrt(jnp.mean(wide**2, -1, keepdims=True) + 1e-6)
    return (wide * scale).astype(jnp.bfloat16)


def layer(h, w):
    a = normed(h)
    gate = jnp.dot(a, w["w_gate"], preferred_element_type=jnp.float32)
    up = jnp.dot(a, w["w_up"], preferred_element_type=jnp.float32)
    return h + matmul((jax.nn.silu(gate) * up).astype(jnp.bfloat16), w["w_down"])


def adamw(w, m, v, g):
    m = 0.9 * m + 0.1 * g
    v = 0.95 * v + 0.05 * g * g
    step = m * lax.rsqrt(v + 1e-8) + 0.1 * w
    return (w - 0.02 * step).astype(jnp.bfloat16), m, v


def stack(weights, h):
    return lax.scan(lambda h, w: (layer(h, w), None), h, weights)[0]


def reference(x, dy, w_gate, w_up, w_down, m_w_gate, m_w_up, m_w_down, v_w_gate, v_w_up, v_w_down):
    weights = dict(zip(NAMES, (w_gate, w_up, w_down), strict=True))

    def take(so_far, sequence):
        h, by_y = sequence
        _, back = jax.vjp(lambda w: stack(w, h), weights)
        return jax.tree.map(lambda total, term: total + term.astype(jnp.float32), so_far, back(by_y)[0]), None

    none_yet = {name: jnp.zeros(w.shape, jnp.float32) for name, w in weights.items()}
    by_weights, _ = lax.scan(take, none_yet, (x, dy))
    gradients = [by_weights[name].astype(jnp.bfloat16).astype(jnp.float32) for name in NAMES]
    new = [
        adamw(w.astype(jnp.float32), m, v, g)
        for w, m, v, g in zip((w_gate, w_up, w_down), (m_w_gate, m_w_up, m_w_down), (v_w_gate, v_w_up, v_w_down), gradients, strict=True)
    ]
    return tuple(one[which] for which in range(3) for one in new)
```

```python
import functools

import jax
import jax.numpy as jnp
from jax import lax
from jax.experimental import pallas as pl
from jax.experimental.pallas import tpu as pltpu
from jax.sharding import PartitionSpec as P

F32, BF16 = jnp.float32, jnp.bfloat16
NN = (((1,), (0,)), ((), ()))
NT = (((1,), (1,)), ((), ()))
LANES = 128
CHUNKS = 2


def dot(a, b, dims):
    return lax.dot_general(a, b, dims, preferred_element_type=F32)


def normed(h):
    wide = h.astype(F32)
    return (wide * lax.rsqrt(jnp.mean(wide * wide, -1, keepdims=True) + 1e-6)).astype(BF16)


def forward_body(part, x_ref, wg_ref, wu_ref, wd_ref, a_ref, h_ref, b_ref, acc):
    x = x_ref[...]
    a = normed(x)
    a_ref[...] = a
    for k in range(wg_ref.shape[1] // part):
        s = slice(k * part, (k + 1) * part)
        gate, up = dot(a, wg_ref[:, s], NN), dot(a, wu_ref[:, s], NN)
        act = (gate * jax.nn.sigmoid(gate) * up).astype(BF16)
        term = dot(act, wd_ref[s, :], NN)
        acc[...] = term if k == 0 else acc[...] + term
    h = x + acc[...].astype(BF16)
    h_ref[...] = h
    b_ref[...] = normed(h)


def forward(x, wg, wu, wd, layer, tile=512, part=512):
    tokens, d = x.shape
    ff = wg.shape[2]
    rows = pl.BlockSpec((tile, d), lambda t: (t, 0))
    whole = lambda a, b: pl.BlockSpec((None, a, b), lambda t: (layer, 0, 0), pipeline_mode=pl.Buffered(1))
    return pl.pallas_call(
        functools.partial(forward_body, part),
        grid=(tokens // tile,),
        in_specs=[rows, whole(d, ff), whole(d, ff), whole(ff, d)],
        out_specs=[rows] * 3,
        out_shape=[jax.ShapeDtypeStruct((tokens, d), BF16)] * 3,
        scratch_shapes=[pltpu.VMEM((tile, d), F32)],
        compiler_params=pltpu.CompilerParams(dimension_semantics=("arbitrary",), vmem_limit_bytes=60 * 2**20),
        cost_estimate=pl.CostEstimate(flops=6 * tokens * d * ff, bytes_accessed=8 * tokens * d + 6 * d * ff, transcendentals=0),
        name="forward",
    )(x, wg, wu, wd)


def backward_body(n, part, need, first, *refs):
    refs = list(refs)
    a_ref, dy_ref = refs[:2]
    wg, wu, wd_ref = refs[2 : 2 + n], refs[2 + n : 2 + 2 * n], refs[2 + 2 * n]
    refs = refs[3 + 2 * n :]
    if need and not first:
        da_in = refs.pop(0)
    if need == 2:
        h_ref = refs.pop(0)
    out = refs.pop(0)
    if need:
        da_out = refs.pop(0)
    wg_t, wu_t, wg_c, wu_c, sum_g, sum_u, sum_d = refs
    t, last = pl.program_id(0), pl.num_programs(0) - 1
    w, d = wg[0].shape[1], a_ref.shape[1]
    units = n * w

    @pl.when(t == 0)
    def _():
        for j in range(n):
            s = slice(j * w, (j + 1) * w)
            for source, turned, plain in ((wg[j], wg_t, wg_c), (wu[j], wu_t, wu_c)):
                value = source[...]
                turned[s, :] = value.T
                if need:
                    plain[:, s] = value
        for total in (sum_g, sum_u, sum_d):
            total[...] = jnp.zeros_like(total)

    a, dy = a_ref[...], dy_ref[...]
    wd = wd_ref[...].reshape(units, d)
    da = None
    for k in range(units // part):
        s = slice(k * part, (k + 1) * part)
        gate, up = dot(wg_t[s, :], a, NT), dot(wu_t[s, :], a, NT)
        d_act = dot(wd[s, :], dy, NT).astype(BF16).astype(F32)
        sig = jax.nn.sigmoid(gate)
        silu = gate * sig
        act = (silu * up).astype(BF16)
        d_up = (d_act * silu).astype(BF16)
        d_gate = (d_act * up * (sig + silu * (1.0 - sig))).astype(BF16)
        sum_d[s, :] += dot(act, dy, NN)
        sum_g[s, :] += dot(d_gate, a, NN)
        sum_u[s, :] += dot(d_up, a, NN)
        if need:
            term = dot(wg_c[:, s], d_gate, NN) + dot(wu_c[:, s], d_up, NN)
            da = term if da is None else da + term
    if need:
        if not first:
            da = da + da_in[...]
        if need == 1:
            da_out[...] = da
        else:
            d_a = da.T.astype(BF16).astype(F32)
            h = h_ref[...].astype(F32)
            scale = lax.rsqrt(jnp.mean(h * h, -1, keepdims=True) + 1e-6)
            d_h = d_a * scale - h * (scale * scale * scale * jnp.mean(d_a * h, -1, keepdims=True))
            da_out[...] = dy + d_h.astype(BF16)

    @pl.when(t == last)
    def _():
        for o in range(n):
            lanes = slice(o * LANES, (o + 1) * LANES)
            out[o, 0:units, :] = sum_g[:, lanes].astype(BF16)
            out[o, units : 2 * units, :] = sum_u[:, lanes].astype(BF16)
            for i in range(d // LANES):
                out[o, 2 * units + i * w : 2 * units + (i + 1) * w, :] = sum_d[o * w : (o + 1) * w, i * LANES : (i + 1) * LANES].astype(BF16)


def backward(n, chunk, layer, a, dy, wg, wu, wd, da, h, need, tile=512, part=512):
    tokens, d = a.shape
    ff = wg.shape[2]
    w = ff // n // CHUNKS
    units = n * w
    first = da is None
    rows, columns = pl.BlockSpec((tile, d), lambda t: (t, 0)), pl.BlockSpec((d, tile), lambda t: (0, t))
    once = pl.Buffered(1)
    column = lambda j: pl.BlockSpec((None, d, w), lambda t: (layer, 0, j * CHUNKS + chunk), pipeline_mode=once)
    ins = [a, dy] + [wg] * n + [wu] * n + [wd.reshape(wd.shape[0], n, ff // n, d)]
    specs = [rows, rows] + [column(j) for j in range(n)] * 2
    specs.append(pl.BlockSpec((None, n, w, d), lambda t: (layer, 0, chunk, 0), pipeline_mode=once))
    outs = [jax.ShapeDtypeStruct((n, 3 * units, LANES), BF16)]
    out_specs = [pl.BlockSpec(outs[0].shape, lambda t: (0, 0, 0), pipeline_mode=once)]
    aliases = {}
    if need and not first:
        if need == 1:
            aliases = {len(ins): 1}
        ins.append(da)
        specs.append(columns)
    if need == 2:
        ins.append(h)
        specs.append(rows)
        outs.append(jax.ShapeDtypeStruct((tokens, d), BF16))
        out_specs.append(rows)
    if need == 1:
        outs.append(jax.ShapeDtypeStruct((d, tokens), F32))
        out_specs.append(columns)
    return pl.pallas_call(
        functools.partial(backward_body, n, part, need, first),
        grid=(tokens // tile,),
        in_specs=specs,
        out_specs=out_specs,
        out_shape=outs,
        scratch_shapes=[pltpu.VMEM((units, d), BF16)] * 2 + [pltpu.VMEM((d, units), BF16)] * 2 + [pltpu.VMEM((units, d), F32)] * 3,
        input_output_aliases=aliases,
        compiler_params=pltpu.CompilerParams(dimension_semantics=("arbitrary",), vmem_limit_bytes=60 * 2**20),
        cost_estimate=pl.CostEstimate(flops=(12 + 4 * bool(need)) * tokens * d * units, bytes_accessed=30 * tokens * d, transcendentals=0),
        name="backward",
    )(*ins)


def adamw(w, m, v, g):
    m = 0.9 * m + 0.1 * g
    v = 0.95 * v + 0.05 * g * g
    step = m * lax.rsqrt(v + 1e-8) + 0.1 * w
    return (w - 0.02 * step).astype(BF16), m, v


def solution(mesh):
    n = mesh.shape["dp"]

    def step(x, dy, wg, wu, wd, *moments):
        layers, d, ff = wg.shape
        w = ff // n // CHUNKS
        units = n * w
        me = lax.axis_index("dp")
        ms, vs = moments[:3], moments[3:]
        inputs, states = [], [x[0]]
        for layer in range(layers - 1):
            a, h, b = forward(states[-1], wg, wu, wd, layer)
            inputs.append(a)
            states.append(h)
        inputs.append(b)
        chunks = {}
        dh = dy[0]
        for layer in reversed(range(layers)):
            da = None
            for chunk in range(CHUNKS):
                need = 0 if layer == 0 else 1 + (chunk == CHUNKS - 1)
                grads, *rest = backward(n, chunk, layer, inputs[layer], dh, wg, wu, wd, da, states[layer], need)
                da = rest[0] if rest else None
                total = lax.psum_scatter(grads, "dp", scatter_dimension=0, tiled=True)[0].astype(F32)
                g = [total[i * units : (i + 1) * units].T.reshape(d // n, n, w) for i in range(2)]
                g.append(jnp.moveaxis(total[2 * units :].reshape(d // LANES, w, LANES), 0, 1).reshape(w, d))
                pick = lambda t: t.reshape(d // n, n, CHUNKS, w)[:, :, chunk]
                cut = lambda i, t: pick(t[layer]) if i < 2 else t[layer].reshape(CHUNKS, w, d)[chunk]
                own = [
                    lax.dynamic_slice(t[layer], (me * (d // n), 0), (d // n, ff)) if i < 2 else lax.dynamic_slice(t[layer], (me * (ff // n), 0), (ff // n, d))
                    for i, t in enumerate((wg, wu, wd))
                ]
                own = [pick(t) if i < 2 else t.reshape(CHUNKS, w, d)[chunk] for i, t in enumerate(own)]
                new = [adamw(own[i].astype(F32), cut(i, ms[i]), cut(i, vs[i]), g[i]) for i in range(3)]
                sent = jnp.concatenate([new[i][0].reshape(-1, d) for i in range(3)])
                everyone = lax.all_gather(sent, "dp", axis=0)
                chunks[layer, chunk] = new, everyone
            dh = da
        outs = []
        for i in range(3):
            rows = (3 * units * LANES) // 3 // d
            parts = [[chunks[layer, c][1][:, i * rows : (i + 1) * rows] for c in range(CHUNKS)] for layer in range(layers)]
            if i < 2:
                whole = [jnp.stack([p.reshape(n, d // n, n, w) for p in ps], 3).reshape(d, ff) for ps in parts]
            else:
                whole = [jnp.stack(ps, 1).reshape(ff, d) for ps in parts]
            outs.append(jnp.stack(whole))
        for which in (1, 2):
            for i in range(3):
                parts = [[chunks[layer, c][0][i][which] for c in range(CHUNKS)] for layer in range(layers)]
                if i < 2:
                    whole = [jnp.stack(ps, 2).reshape(d // n, ff) for ps in parts]
                else:
                    whole = [jnp.concatenate(ps) for ps in parts]
                outs.append(jnp.stack(whole))
        return tuple(outs)

    batch, split = P(("rep", "dp"), None, None), P(None, "dp", None)
    return jax.shard_map(
        step,
        mesh=mesh,
        in_specs=(batch, batch) + (P(),) * 3 + (split,) * 6,
        out_specs=(P("rep", None, None),) * 3 + (P("rep", "dp", None),) * 6,
        check_vma=False,
    )
```

```python
import functools

import jax
import jax.numpy as jnp
from jax import lax
from jax.experimental import pallas as pl
from jax.experimental.pallas import tpu as pltpu
from jax.sharding import PartitionSpec as P


F32, BF16 = jnp.float32, jnp.bfloat16
NN = (((1,), (0,)), ((), ()))
NT = (((1,), (1,)), ((), ()))
LANES = 128
HALF = 2
LAST, EARLIER = ((8, 0), (8, 1), (4, 1), (4, 2), (4, 3)), ((4, 0), (4, 1), (4, 2), (4, 3))


def dot(a, b, dims):
    return lax.dot_general(a, b, dims, preferred_element_type=F32)


def normed(h):
    wide = h.astype(F32)
    return (wide * lax.rsqrt(jnp.mean(wide * wide, -1, keepdims=True) + 1e-6)).astype(BF16)


def sigmoid(t):
    return 0.5 * jnp.tanh(0.5 * t) + 0.5


def forward_body(part, x_ref, wg_ref, wu_ref, wd_ref, a_ref, h_ref, b_ref, acc):
    x = x_ref[...]
    a = normed(x)
    a_ref[...] = a
    for k in range(wg_ref.shape[1] // part):
        s = slice(k * part, (k + 1) * part)
        gate, up = dot(a, wg_ref[:, s], NN), dot(a, wu_ref[:, s], NN)
        act = (gate * sigmoid(gate) * up).astype(BF16)
        term = dot(act, wd_ref[s, :], NN)
        acc[...] = term if k == 0 else acc[...] + term
    h = x + acc[...].astype(BF16)
    h_ref[...] = h
    b_ref[...] = normed(h)


def forward(x, wg, wu, wd, layer, tile=512, part=512):
    tokens, d = x.shape
    ff = wg.shape[2]
    rows = pl.BlockSpec((tile, d), lambda t: (t, 0))
    whole = lambda a, b: pl.BlockSpec((None, a, b), lambda t: (layer, 0, 0), pipeline_mode=pl.Buffered(1))
    return pl.pallas_call(
        functools.partial(forward_body, part),
        grid=(tokens // tile,),
        in_specs=[rows, whole(d, ff), whole(d, ff), whole(ff, d)],
        out_specs=[rows] * 3,
        out_shape=[jax.ShapeDtypeStruct((tokens, d), BF16)] * 3,
        scratch_shapes=[pltpu.VMEM((tile, d), F32)],
        compiler_params=pltpu.CompilerParams(dimension_semantics=("arbitrary",), vmem_limit_bytes=60 * 2**20),
        cost_estimate=pl.CostEstimate(flops=6 * tokens * d * ff, bytes_accessed=8 * tokens * d + 6 * d * ff, transcendentals=0),
        name="forward",
    )(x, wg, wu, wd)


def backward_body(n, part, need, first, waits, *refs):
    refs = list(refs)[waits:]
    a_ref, dy_ref = refs[:2]
    wg, wu, wd_ref = refs[2 : 2 + n], refs[2 + n : 2 + 2 * n], refs[2 + 2 * n]
    refs = refs[3 + 2 * n :]
    if need and not first:
        da_in = refs.pop(0)
    if need == 2:
        h_ref = refs.pop(0)
    out = refs.pop(0)
    if need:
        da_out = refs.pop(0)
    wg_t, wu_t, wg_c, wu_c, sum_g, sum_u, sum_d = refs
    t, last = pl.program_id(0), pl.num_programs(0) - 1
    w, d = wg[0].shape[1], a_ref.shape[1]
    units = n * w

    @pl.when(t == 0)
    def _():
        for j in range(n):
            s = slice(j * w, (j + 1) * w)
            for source, turned, plain in ((wg[j], wg_t, wg_c), (wu[j], wu_t, wu_c)):
                value = source[...]
                turned[s, :] = value.T
                if need:
                    plain[:, s] = value
        for total in (sum_g, sum_u, sum_d):
            total[...] = jnp.zeros_like(total)

    a, dy = a_ref[...], dy_ref[...]
    wd = wd_ref[...].reshape(units, d)
    da = None
    for k in range(units // part):
        s = slice(k * part, (k + 1) * part)
        gate, up = dot(wg_t[s, :], a, NT), dot(wu_t[s, :], a, NT)
        d_act = dot(wd[s, :], dy, NT).astype(BF16).astype(F32)
        sig = sigmoid(gate)
        silu = gate * sig
        act = (silu * up).astype(BF16)
        d_up = (d_act * silu).astype(BF16)
        d_gate = (d_act * up * (sig + silu * (1.0 - sig))).astype(BF16)
        sum_d[s, :] += dot(act, dy, NN)
        sum_g[s, :] += dot(d_gate, a, NN)
        sum_u[s, :] += dot(d_up, a, NN)
        if need:
            term = dot(wg_c[:, s], d_gate, NN) + dot(wu_c[:, s], d_up, NN)
            da = term if da is None else da + term
    if need:
        if not first:
            da = da + da_in[...]
        if need == 1:
            da_out[...] = da
        else:
            d_a = da.T.astype(BF16).astype(F32)
            h = h_ref[...].astype(F32)
            scale = lax.rsqrt(jnp.mean(h * h, -1, keepdims=True) + 1e-6)
            d_h = d_a * scale - h * (scale * scale * scale * jnp.mean(d_a * h, -1, keepdims=True))
            da_out[...] = dy + d_h.astype(BF16)

    @pl.when(t == last)
    def _():
        for o in range(n):
            lanes = slice(o * LANES, (o + 1) * LANES)
            out[o, 0:units, :] = sum_g[:, lanes].astype(BF16)
            out[o, units : 2 * units, :] = sum_u[:, lanes].astype(BF16)
            for i in range(d // LANES):
                out[o, 2 * units + i * w : 2 * units + (i + 1) * w, :] = sum_d[o * w : (o + 1) * w, i * LANES : (i + 1) * LANES].astype(BF16)


def backward(n, share, layer, a, dy, wg, wu, wd, da, h, need, after, tile=512, part=512):
    tokens, d = a.shape
    ff = wg.shape[2]
    pieces, chunk = share
    w = ff // n // pieces
    units = n * w
    first = da is None
    rows, columns = pl.BlockSpec((tile, d), lambda t: (t, 0)), pl.BlockSpec((d, tile), lambda t: (0, t))
    once = pl.Buffered(1)
    column = lambda j: pl.BlockSpec((None, d, w), lambda t: (layer, 0, j * pieces + chunk), pipeline_mode=once)
    ins = list(after) + [a, dy] + [wg] * n + [wu] * n + [wd.reshape(wd.shape[0], n, ff // n, d)]
    specs = [pl.BlockSpec(memory_space=pl.ANY)] * len(after) + [rows, rows] + [column(j) for j in range(n)] * 2
    specs.append(pl.BlockSpec((None, n, w, d), lambda t: (layer, 0, chunk, 0), pipeline_mode=once))
    outs = [jax.ShapeDtypeStruct((n, 3 * units, LANES), BF16)]
    out_specs = [pl.BlockSpec(outs[0].shape, lambda t: (0, 0, 0), pipeline_mode=once)]
    aliases = {}
    if need and not first:
        if need == 1:
            aliases = {len(ins): 1}
        ins.append(da)
        specs.append(columns)
    if need == 2:
        ins.append(h)
        specs.append(rows)
        outs.append(jax.ShapeDtypeStruct((tokens, d), BF16))
        out_specs.append(rows)
    if need == 1:
        outs.append(jax.ShapeDtypeStruct((d, tokens), F32))
        out_specs.append(columns)
    return pl.pallas_call(
        functools.partial(backward_body, n, part, need, first, len(after)),
        grid=(tokens // tile,),
        in_specs=specs,
        out_specs=out_specs,
        out_shape=outs,
        scratch_shapes=[pltpu.VMEM((units, d), BF16)] * 2 + [pltpu.VMEM((d, units), BF16)] * 2 + [pltpu.VMEM((units, d), F32)] * 3,
        input_output_aliases=aliases,
        compiler_params=pltpu.CompilerParams(dimension_semantics=("arbitrary",), vmem_limit_bytes=60 * 2**20),
        cost_estimate=pl.CostEstimate(flops=(12 + 4 * bool(need)) * tokens * d * units, bytes_accessed=30 * tokens * d, transcendentals=0),
        name="backward",
    )(*ins)


def adamw(w, m, v, g):
    m = 0.9 * m + 0.1 * g
    v = 0.95 * v + 0.05 * g * g
    step = m * lax.rsqrt(v + 1e-8) + 0.1 * w
    return (w - 0.02 * step).astype(BF16), m, v


def update_body(kept, waits, me_ref, *refs):
    g, w, m, v = (refs[3 * i : 3 * i + 3] for i in range(4))
    sent, *new = refs[12 + kept + waits :]
    for i in range(3):
        grad = g[i][...].astype(F32)
        if i < 2:
            grad = grad.T
        one, new[i][...], new[3 + i][...] = adamw(w[i][...].astype(F32), m[i][...], v[i][...], grad)
        if i < 2:
            sent[i] = one
        else:
            for q in range(one.shape[0] // LANES):
                sent[i, :, q * LANES : (q + 1) * LANES] = one[q * LANES : (q + 1) * LANES]


def update(me, n, share, layer, total, weights, ms, vs, done, after):
    pieces, chunk = share
    _, _, ff = weights[0].shape
    w = ff // n // pieces
    grad = [pl.BlockSpec((w, LANES), functools.partial(lambda i, j, me: (i * n + j, 0), i)) for i in range(3)]
    across = pl.BlockSpec((None, LANES, w), lambda j, me: (layer, 0, j * pieces + chunk))
    down = pl.BlockSpec((None, w, LANES), lambda j, me: (layer, chunk, j))
    own = pl.BlockSpec((None, LANES, w), lambda j, me: (layer, me[0], j * pieces + chunk))
    own_down = pl.BlockSpec((None, w, LANES), lambda j, me: (layer, me[0] * pieces + chunk, j))
    moments = [across, across, down] * 2
    ins = [total] * 3 + list(weights) + list(ms) + list(vs) + list(done) + list(after)
    specs = grad + [own, own, own_down] + moments + [pl.BlockSpec(memory_space=pl.ANY)] * (len(done) + len(after))
    return pl.pallas_call(
        functools.partial(update_body, len(done), len(after)),
        grid_spec=pltpu.PrefetchScalarGridSpec(
            num_scalar_prefetch=1,
            grid=(n,),
            in_specs=specs,
            out_specs=[pl.BlockSpec((None, 3, LANES, w), lambda j, me: (j, 0, 0, 0))] + moments,
        ),
        out_shape=[jax.ShapeDtypeStruct((n, 3, LANES, w), BF16)] + [jax.ShapeDtypeStruct(t.shape, F32) for t in (*ms, *vs)],
        input_output_aliases={13 + i: 1 + i for i in range(len(done))},
        compiler_params=pltpu.CompilerParams(dimension_semantics=("arbitrary",)),
        cost_estimate=pl.CostEstimate(flops=8 * 10**9, bytes_accessed=60 * LANES * n * w, transcendentals=0),
        name="update",
    )(me, *ins)


def place_body(n, pieces, chunk, layer, kept, me_ref, own, right, left, far_a, far_b, *refs):
    outs, done = refs[kept : kept + 3], refs[-1]
    w, near = own.shape[3], n // HALF
    copies = []
    for r in range(n):
        owner = lax.rem(me_ref[0] + r, n)
        rows = pl.ds(pl.multiple_of(owner * LANES, LANES), LANES)
        for j in range(n):
            ref, at = {0: (own, j), 1: (right, j), n - 1: (left, j)}.get(r, (far_a, j) if j < near else (far_b, j - near))
            columns = pl.ds((j * pieces + chunk) * w, w)
            copies += [(ref.at[at, i], outs[i].at[layer, rows, columns]) for i in range(2)]
            for q in range(w // LANES):
                part = pl.ds(pl.multiple_of((owner * pieces + chunk) * w + q * LANES, LANES), LANES)
                copies.append((ref.at[at, 2, :, q * LANES : (q + 1) * LANES], outs[2].at[layer, part, j * LANES : (j + 1) * LANES]))
    copies = [pltpu.make_async_copy(a, b, done.at[i]) for i, (a, b) in enumerate(copies)]
    for copy in copies:
        copy.start()
    for copy in copies:
        copy.wait()


def place(me, n, share, layer, blocks, weights, done):
    pieces, chunk = share
    _, d, ff = weights[0].shape
    w = ff // n // pieces
    here, anywhere = pl.BlockSpec(memory_space=pltpu.VMEM), pl.BlockSpec(memory_space=pl.ANY)
    return pl.pallas_call(
        functools.partial(place_body, n, pieces, chunk, layer, len(done)),
        in_specs=[pl.BlockSpec(memory_space=pltpu.SMEM)] + [here] * len(blocks) + [anywhere] * len(done),
        out_specs=[anywhere] * 3,
        out_shape=[jax.ShapeDtypeStruct(t.shape, BF16) for t in weights],
        scratch_shapes=[pltpu.SemaphoreType.DMA((n * n * (2 + w // LANES),))],
        input_output_aliases={1 + len(blocks) + i: i for i in range(len(done))},
        cost_estimate=pl.CostEstimate(flops=4 * 10**9, bytes_accessed=12 * d * w, transcendentals=0),
        name="place",
    )(me, *blocks, *done)


def solution(mesh):
    n = mesh.shape["dp"]
    to_right = [(i, (i + 1) % n) for i in range(n)]
    to_left = [(i, (i - 1) % n) for i in range(n)]

    def work(x, dy, wg, wu, wd, *moments):
        layers, d, _ = wg.shape
        assert d == n * LANES and n == 2 * HALF
        weights = (wg, wu, wd)
        me = lax.axis_index("dp")[None].astype(jnp.int32)
        ms, vs = moments[:3], moments[3:]
        inputs, states = [], [x[0]]
        for layer in range(layers - 1):
            a, h, b = forward(states[-1], wg, wu, wd, layer)
            inputs.append(a)
            states.append(h)
        inputs.append(b)
        shares = [(layer, s) for layer in reversed(range(layers)) for s in (LAST if layer == layers - 1 else EARLIER)]
        count = len(shares)
        total, sent, near, new, placed = {}, {}, {}, (), ()

        def send(t, pairs):
            return lax.ppermute(t, "dp", pairs)

        def renew(i, new, after):
            layer, share = shares[i]
            sent[i], *new = update(me, n, share, layer, total[i], weights, ms, vs, new, after)
            near[i] = [send(sent[i], p) for p in (to_right, to_left)]
            return new

        def relay(i):
            half = n // HALF
            first = near[i][0][:half], near[i][1][half:]
            near[i] += [send(first[j], p) for j, p in enumerate((to_right, to_left))]
            return list(first)

        def settle(i, placed):
            layer, share = shares[i]
            from_left, from_right, far_a, far_b = near[i]
            return place(me, n, share, layer, [sent[i], from_right, from_left, far_a, far_b], weights, placed)

        dh, da = dy[0], None
        for k, (layer, share) in enumerate(shares):
            after = []
            if k >= 2:
                new = renew(k - 2, new, [])
                after.append(sent[k - 2])
            if k >= 3:
                after += relay(k - 3)
            if k >= 4:
                placed = settle(k - 4, placed)
                after.append(placed[0])
            final = k + 1 == count or shares[k + 1][0] != layer
            need = 0 if layer == 0 else 1 + final
            grads, *rest = backward(n, share, layer, inputs[layer], dh, wg, wu, wd, da, states[layer], need, after)
            da = rest[0] if rest else None
            total[k] = lax.psum_scatter(grads, "dp", scatter_dimension=0, tiled=True)[0]
            if final:
                dh, da = da, None
        for i in (count - 2, count - 1):
            after = relay(i - 1)
            placed = settle(i - 2, placed)
            new = renew(i, new, after + [placed[0]])
        relay(count - 1)
        for i in (count - 2, count - 1):
            placed = settle(i, placed)
        return (*placed, *new)

    batch, split = P(("rep", "dp"), None, None), P(None, "dp", None)
    return jax.shard_map(
        work,
        mesh=mesh,
        in_specs=(batch, batch) + (P(),) * 3 + (split,) * 6,
        out_specs=(P("rep", None, None),) * 3 + (P("rep", "dp", None),) * 6,
        check_vma=False,
    )
```
